32 devices in a mesh: dp: 4 (over y, x), expert: 4 (over z), tensor: 2 (over core).
Axes of the slice: x: 2, y: 2, z: 4, core: 2. Of those that a mesh axis runs over, the one named last changes fastest.
Arguments:
- out_grad: bfloat16 [2048, 2048], P(('dp', 'expert'), 'tensor'), may hold values from -6 to 6
- seq_ids: int32 [16, 128], P(('dp', 'expert')), may hold values from 0 to 3, never falling along the last dimension, each value on 1 to 64 neighbouring positions
- seq_weights: float32 [16, 4], P(('dp', 'expert')), may hold values from -1.5 to 1.5
- expert_ids: int32 [2048, 2], P(('dp', 'expert')), may hold values from 0 to 3, all different within a row; in each aligned block of 128 rows (0 to 127, 128 to 255, ...) at most 96 rows name the same one
- route_probs: bfloat16 [2048, 2], P(('dp', 'expert')), may hold values from 0.19921875 to 1
- down_weight: bfloat16 [4, 7168, 2048], P('expert', ('dp', 'tensor')), may hold values from -0.0625 to 0.0625
- gate_pre: bfloat16 [4, 7168, 1536], P('expert', ('dp', 'tensor')), may hold values from -6 to 6
- up_pre: bfloat16 [4, 7168, 1536], P('expert', ('dp', 'tensor')), may hold values from -6 to 6
Outputs:
- grad_gate: bfloat16 [4, 7168, 1536], P('expert', ('dp', 'tensor'))
- grad_up: bfloat16 [4, 7168, 1536], P('expert', ('dp', 'tensor'))
- grad_down: bfloat16 [4, 7168, 2048], P('expert', ('dp', 'tensor'))
- grad_probs: float32 [2048, 2], P(('dp', 'expert'))
The draws below stay inside these ranges and needn't reach their ends.
Inputs may be any that keep to these rules, and one draw needn't show every extreme that they name: `expert_ids`: the two experts of a token differ. Among the 128 tokens of one shard no expert is named more than 96 times, and in every draw some expert is named exactly 96 times by the tokens of some shard. `seq_ids`: along a shard's row the ids never fall; each of the 4 ids names 1 to 64 tokens of the row, and one names exactly 64.
All inputs are finite; a program needn't handle non-finite values.
Results may differ from the reference program's by a relative error of at most 0.0064.
Values may be sent and summed in bfloat16 or wider, within the bound.
A program may use at most 128 MiB of HBM per device.

```python
import math
import jax
import jax.numpy as jnp
import numpy as np
from jax import lax

D = 2048
FF = 7168
TOK_DEV = 128
SEQ_DEV = 4
EXPERTS = 4
SHARDS = 16
TOKENS = 2048
CAP = 96
SLOTS = 1536


def shard_levels(stream_key, dims, cuts, least, high):
    level, own = 1.0, jax.random.fold_in(stream_key, 6)
    for axis_at, shards_of in cuts:
        heights = jnp.exp(jax.random.uniform(jax.random.fold_in(own, axis_at), (shards_of,), jnp.float32, least / len(cuts), high / len(cuts)))
        level = level * jnp.repeat(heights, dims[axis_at] // shards_of).reshape([-1 if axis == axis_at else 1 for axis in range(len(dims))])
    return level


def length_profile(amount, total, reach, slope):
    loads = [(1 << 20) // math.isqrt(grade ** slope) + 1 for grade in range(2, amount + 1)]
    spare, counts = total - reach - (amount - 1), [1] * (amount - 1)
    while spare > 0:
        candidates = [i for i in range(amount - 1) if counts[i] < reach]
        mass, budget = sum([loads[i] for i in candidates]), spare
        for i in candidates:
            more = min(reach - counts[i], max(1, budget * loads[i] // mass), spare)
            counts[i] = counts[i] + more
            spare = spare - more
    return np.array([reach] + counts)


def ragged(rng, amount, total, bound, slope):
    if amount == 2:
        one = jax.random.randint(rng, (), max(1, total - bound), min(bound, total - 1) + 1)
        return jnp.stack([one, total - one])
    lengths = jnp.asarray(length_profile(amount, total, bound, slope), jnp.int32)
    pairs = (amount - 1) // 2
    giver, receiver = lengths[1:1 + 2 * pairs:2], lengths[2:2 + 2 * pairs:2]
    slack = jnp.minimum(giver - 1, bound - receiver)
    shifted = jax.random.randint(jax.random.fold_in(rng, 1), (pairs,), 0, 1 << 20) % (slack + 1)
    lengths = lengths.at[1:1 + 2 * pairs:2].set(giver - shifted).at[2:2 + 2 * pairs:2].set(receiver + shifted)
    return lengths[jax.random.permutation(jax.random.fold_in(rng, 2), amount)]


def shared_out(stream_key, own, number, rows, amount, top, limit, skew):
    ranking = jax.random.permutation(stream_key, amount)
    heavy_load, ordinary = load_shares(amount, rows * top, limit, skew, True), load_shares(amount, rows * top, limit, skew, False)
    places = jnp.arange(amount)

    def named(lengths, offset_by):
        used = int((lengths > 0).sum())
        fixed = max(1, used // 4)
        moved = fixed + (places - fixed + offset_by * (used - fixed)) % max(1, amount - fixed)
        return jnp.zeros((amount,), jnp.int32).at[ranking[jnp.where(places < fixed, places, moved)]].set(jnp.asarray(lengths, jnp.int32))

    lengths = jnp.where(number % 4 == 0, named(heavy_load, number // 4), named(ordinary, number - number // 4 - 1))
    mixed = jax.random.permutation(jax.random.fold_in(own, 3), amount)
    giver, sink = mixed[0:amount // 2 * 2:2], mixed[1:amount // 2 * 2:2]
    slack = jnp.minimum(lengths[giver] - 1, limit - lengths[sink]) // 2
    slack = jnp.where((giver == ranking[0]) | (sink == ranking[0]) | (lengths[sink] == 0), 0, jnp.maximum(slack, 0))
    moved = jax.random.randint(jax.random.fold_in(own, 4), (amount // 2,), 0, 1 << 20) % (slack + 1)
    lengths = lengths.at[giver].add(-moved).at[sink].add(moved)
    labels = jnp.searchsorted(jnp.cumsum(lengths), jnp.arange(rows * top), side="right").astype(jnp.int32)
    listing = labels.reshape(top, rows).T
    listing = listing[jax.random.permutation(jax.random.fold_in(own, 1), rows)]
    offset_by = jax.random.randint(jax.random.fold_in(own, 2), (rows, 1), 0, top)
    return jnp.take_along_axis(listing, (jnp.arange(top)[None, :] + offset_by) % top, axis=1)


def load_shares(count, total, bound, slope, full):
    loads = [(1 << 20) // math.isqrt(rank ** slope) + 1 for rank in range(1, count + 1)]
    largest = bound if full else min(bound, max(-(-total // count), total * loads[0] // sum(loads)))
    least = 1 if total - largest >= count - 1 else 0
    given, rest = [largest] + [least] * (count - 1), total - largest - least * (count - 1)
    while rest > 0:
        movable = [i for i in range(1, count) if given[i] < largest] or [i for i in range(1, count) if given[i] < bound]
        mass, left = sum([loads[i] for i in movable]), rest
        for i in movable:
            addition = min(bound - given[i], max(1, left * loads[i] // mass), rest)
            given[i] = given[i] + addition
            rest = rest - addition
    return np.array(given)


def gaussian(own_key, shape, scale, most, cuts=(), held_as=jnp.bfloat16):
    drawn = jax.random.normal(own_key, shape, jnp.float32) * scale
    if len(cuts) > 0:
        drawn = shard_levels(own_key, shape, cuts, -0.22, 0.18) * drawn
    return jnp.clip(drawn, min=-most, max=most).astype(held_as)


def setup_inputs(seed: int = 0) -> dict:
    key_list = jax.random.split(jax.random.key(seed), 9)
    out_grad = gaussian(key_list[0], (TOKENS, D), 0.5, 6.0, ((0, 16), (1, 2)))
    seq_ids = jax.vmap(lambda own: jnp.searchsorted(jnp.cumsum(ragged(own, SEQ_DEV, TOK_DEV, TOK_DEV // 2, 0)), jnp.arange(TOK_DEV), side="right"))(jax.random.split(key_list[1], SHARDS)).reshape((SHARDS, TOK_DEV)).astype(jnp.int32)
    seq_weights = jnp.clip(jax.random.uniform(key_list[2], (SHARDS, SEQ_DEV), jnp.float32, -1.5, 1.5) * shard_levels(key_list[2], (SHARDS, SEQ_DEV), ((0, 16),), -0.4, 0.0), -1.5, 1.5)
    expert_ids_keys = jax.random.split(jax.random.fold_in(key_list[3], 1), TOKENS // TOK_DEV)
    expert_ids_turns = jax.random.permutation(jax.random.fold_in(key_list[3], 3), TOKENS // TOK_DEV)
    expert_ids = jax.vmap(lambda own, number: shared_out(jax.random.fold_in(key_list[3], 2), own, number, TOK_DEV, EXPERTS, 2, CAP, 2))(expert_ids_keys, expert_ids_turns).reshape((TOKENS, 2))
    route_probs = jnp.clip(0.19921875 + 0.80078125 * jax.random.uniform(key_list[4], (TOKENS, 2), jnp.float32) ** shard_levels(key_list[4], (TOKENS, 2), ((0, 16),), -0.2, 0.2), 0.19921875, 1.0).astype(jnp.bfloat16)
    down_weight = gaussian(key_list[5], (EXPERTS, FF, D), FF ** -0.5, 0.0625, ((0, 4), (1, 8)))
    gate_pre = gaussian(key_list[6], (EXPERTS, FF, SLOTS), 1.0, 6.0, ((0, 4), (1, 8)))
    up_pre = gaussian(key_list[7], (EXPERTS, FF, SLOTS), 1.0, 6.0, ((0, 4), (1, 8)))
    return {"out_grad": out_grad, "seq_ids": seq_ids, "seq_weights": seq_weights, "expert_ids": expert_ids, "route_probs": route_probs, "down_weight": down_weight, "gate_pre": gate_pre, "up_pre": up_pre}


def silu_parts(pre_act):
    logistic = jax.nn.sigmoid(pre_act)
    return pre_act * logistic, logistic * (1.0 + pre_act * (1.0 - logistic))


def reference(out_grad, seq_ids, seq_weights, expert_ids, route_probs, down_weight, gate_pre, up_pre):
    shards = seq_ids.shape[0]
    token_count = seq_ids.shape[1]
    experts = down_weight.shape[0]
    capacity = gate_pre.shape[2] // shards
    feature_width = out_grad.shape[1]
    weight_tok = jnp.take_along_axis(seq_weights, seq_ids, axis=1).reshape(-1)
    scaled = (weight_tok[:, None] * out_grad.astype(jnp.float32)).astype(jnp.bfloat16)
    chosen = expert_ids.reshape(shards, 2 * token_count)
    onehot = (chosen[:, :, None] == jnp.arange(experts, dtype=jnp.int32)[None, None, :]).astype(jnp.int32)
    earlier = (jnp.cumsum(onehot, axis=1) - onehot).astype(jnp.int32)
    position = jnp.sum(earlier * onehot, axis=2).astype(jnp.int32)
    slot_index = (jnp.arange(shards, dtype=jnp.int32)[:, None] * capacity + position).reshape(-1).astype(jnp.int32)
    chosen_flat = chosen.reshape(-1).astype(jnp.int32)
    pair_rows = jnp.repeat(scaled, 2, axis=0)
    prob_flat = route_probs.reshape(-1)
    row_table = jnp.zeros((experts, shards * capacity, feature_width), jnp.bfloat16).at[chosen_flat, slot_index].set(pair_rows)
    prob_table = jnp.zeros((experts, shards * capacity), jnp.bfloat16).at[chosen_flat, slot_index].set(prob_flat)

    def per_expert(operands):
        expert_rows, expert_probs, expert_weight, gate_block, up_block = operands
        activated, derivative = silu_parts(gate_block.astype(jnp.float32))
        up_float = up_block.astype(jnp.float32)
        hidden = (activated * up_float).astype(jnp.bfloat16)
        upstream = lax.dot_general(expert_weight, expert_rows, (((1,), (1,)), ((), ())), preferred_element_type=jnp.float32)
        probe_part = jnp.sum(upstream * hidden.astype(jnp.float32), axis=0)
        factor = expert_probs.astype(jnp.float32)[None, :]
        grad_hidden = factor * upstream
        gate_out = (grad_hidden * up_float * derivative).astype(jnp.bfloat16)
        up_out = (grad_hidden * activated).astype(jnp.bfloat16)
        weighted = (expert_probs.astype(jnp.float32)[:, None] * expert_rows.astype(jnp.float32)).astype(jnp.bfloat16)
        down_out = jnp.dot(hidden, weighted, preferred_element_type=jnp.float32).astype(jnp.bfloat16)
        return gate_out, up_out, down_out, probe_part

    grad_gate, grad_up, grad_down, probe = lax.map(per_expert, (row_table, prob_table, down_weight, gate_pre, up_pre))
    grad_probs = probe[chosen_flat, slot_index].reshape(-1, 2)
    return grad_gate, grad_up, grad_down, grad_probs
```

```python
import functools

import jax
import jax.numpy as jnp
from jax import lax
from jax.experimental import pallas as pl
from jax.experimental.pallas import tpu as pltpu
from jax.sharding import PartitionSpec as P

MESH = pl.DeviceIdType.MESH
LANES = 128
SUBLANES = 8


def silu_parts(pre_act):
    logistic = jax.nn.sigmoid(pre_act)
    return (pre_act * logistic, logistic * (1.0 + pre_act * (1.0 - logistic)))


def flip(index, mask):
    bit = 1
    while bit <= mask:
        if mask & bit:
            index = index + bit * (1 - 2 * lax.rem(lax.div(index, bit), 2))
        bit *= 2
    return index


class Copies:
    def __init__(self, send_sem, recv_sem):
        self.send_sem, self.recv_sem, self.made = send_sem, recv_sem, []

    def start(self, src, dst, device):
        at = len(self.made)
        copy = pltpu.make_async_remote_copy(
            src_ref=src,
            dst_ref=dst,
            send_sem=self.send_sem.at[at],
            recv_sem=self.recv_sem.at[at],
            device_id=device,
            device_id_type=MESH,
        )
        copy.start()
        self.made.append(copy)
        return copy


def greet(peers):
    barrier = pltpu.get_barrier_semaphore()
    for peer in peers:
        pl.semaphore_signal(barrier, inc=1, device_id=peer, device_id_type=MESH)
    pl.semaphore_wait(barrier, len(peers))


def copy_count(columns, experts, cores):
    if columns == 4:
        per_block = 6 + 7 * (cores - 1)
        return (experts - 1) * 2 + (columns - 1) + experts * per_block
    return (experts - 1) * 2 + (columns - 1) * 2 + columns * (cores - 1)


def gather_kernel(
    columns, experts, cores, rows_ref, probs_ref, out_ref, probs_out, send_sem, recv_sem
):
    d, e, t = lax.axis_index("dp"), lax.axis_index("expert"), lax.axis_index("tensor")
    half = rows_ref.shape[2]
    peers = (
        [(d, flip(e, k), t) for k in range(1, experts)]
        + [(flip(d, m), e, t) for m in range(1, columns)]
        + [(d, e, flip(t, f)) for f in range(1, cores)]
    )
    greet(peers)
    copies = Copies(send_sem, recv_sem)
    base = pl.multiple_of(t * half, half)
    mine = pl.ds(base, half)
    along, small = [None], [None]
    for k in range(1, experts):
        to = (d, flip(e, k), t)
        along.append(copies.start(rows_ref.at[flip(e, k)], out_ref.at[d, e, :, mine], to))
        small.append(copies.start(probs_ref.at[flip(e, k)], probs_out.at[d, e], to))

    def to_cores(src, dst):
        return [copies.start(src, dst, (d, e, flip(t, f))) for f in range(1, cores)]

    last = []
    if columns == 4:
        piece = half // 2
        cuts = [pl.ds(pl.multiple_of(base + p * piece, piece), piece) for p in range(2)]
        sent = {}

        def spread(k):
            origin = flip(e, k)
            if k > 0:
                along[k].wait_recv()
            for m, order in ((1, (0, 1)), (2, (1, 0))):
                for p in order:
                    here = out_ref.at[d, origin, :, cuts[p]]
                    src = rows_ref.at[e, :, pl.ds(p * piece, piece)] if k == 0 else here
                    sent[k, m, p] = copies.start(src, here, (flip(d, m), e, t))
            whole = out_ref.at[d, origin, :, mine]
            last.extend(to_cores(rows_ref.at[e] if k == 0 else whole, whole))

        def forward(k):
            origin = flip(e, k)
            for m, p in ((1, 0), (2, 1)):
                sent[k, m, p].wait_recv()
                block = out_ref.at[flip(d, m), origin, :, cuts[p]]
                sent[k, 3, p] = copies.start(block, block, (flip(d, 3 - m), e, t))
                last.extend(to_cores(block, block))
            for m, p in ((1, 1), (2, 0)):
                sent[k, m, p].wait_recv()
                block = out_ref.at[flip(d, m), origin, :, cuts[p]]
                last.extend(to_cores(block, block))

        def finish(k):
            for p in range(2):
                sent[k, 3, p].wait_recv()
                block = out_ref.at[flip(d, 3), flip(e, k), :, cuts[p]]
                last.extend(to_cores(block, block))

        spread(0)
        out_ref[d, e, :, mine] = rows_ref[e]
        probs_out[d, e] = probs_ref[e]
        for k in range(1, experts):
            spread(k)
            forward(k - 1)
            if k > 1:
                finish(k - 2)
        forward(experts - 1)
        if experts > 1:
            finish(experts - 2)
        finish(experts - 1)
    else:
        out_ref[d, e, :, mine] = rows_ref[e]
        probs_out[d, e] = probs_ref[e]
        for k in range(1, experts):
            along[k].wait_recv()
        group = out_ref.at[d, :, :, mine]
        spreads = [copies.start(group, group, (flip(d, m), e, t)) for m in range(1, columns)]
        last.extend(to_cores(group, group))
        for m in range(1, columns):
            spreads[m - 1].wait_recv()
            block = out_ref.at[flip(d, m), :, :, mine]
            last.extend(to_cores(block, block))
    for k in range(1, experts):
        small[k].wait_recv()
    group = probs_out.at[d]
    for m in range(1, columns):
        last.append(copies.start(group, group, (flip(d, m), e, t)))
    for copy in last:
        copy.wait_recv()
    for copy in copies.made:
        copy.wait_send()


def probe_kernel(columns, experts, cores, part_ref, out_ref, first, total, second, send_sem, recv_sem):
    d, e, t = lax.axis_index("dp"), lax.axis_index("expert"), lax.axis_index("tensor")
    others = [(m, f) for m in range(columns) for f in range(cores) if m or f]
    greet(
        [(flip(d, m), e, flip(t, f)) for m, f in others]
        + [(d, flip(e, k), t) for k in range(1, experts)]
    )
    copies = Copies(send_sem, recv_sem)
    for at, (m, f) in enumerate(others):
        to = (flip(d, m), e, flip(t, f))
        copies.start(part_ref.at[flip(d, m)], first.at[at], to)
    acc = part_ref[d]
    for at in range(len(others)):
        copies.made[at].wait_recv()
        acc = acc + first[at]
    total[...] = acc
    backs = [copies.start(total, second.at[k - 1], (d, flip(e, k), t)) for k in range(1, experts)]
    out_ref[...] = jnp.zeros_like(out_ref)
    out_ref[pl.ds(e, 1), :] = total[pl.ds(e, 1), :]
    for k in range(1, experts):
        backs[k - 1].wait_recv()
        out_ref[pl.ds(flip(e, k), 1), :] = second[k - 1, pl.ds(e, 1), :]
    for copy in copies.made:
        copy.wait_send()


def local(out_grad, seq_ids, seq_weights, expert_ids, route_probs, down_weight, gate_pre, up_pre):
    experts = lax.axis_size("expert")
    columns = lax.axis_size("dp")
    cores = lax.axis_size("tensor")
    token_count = seq_ids.shape[1]
    slots = gate_pre.shape[2]
    capacity = slots // (columns * experts)
    half_width = out_grad.shape[1]
    width = half_width * cores
    seq_count = seq_weights.shape[1]
    block_size = experts * capacity
    padded = -(-capacity // LANES) * LANES
    depth = -(-experts // SUBLANES) * SUBLANES
    gate_local = gate_pre[0]
    up_local = up_pre[0]
    weight_local = down_weight[0]
    member = (seq_ids[0][:, None] == jnp.arange(seq_count, dtype=jnp.int32)[None, :]).astype(
        jnp.float32
    )
    weight_tok = jnp.sum(member * seq_weights[0][None, :], axis=1)
    scaled = (weight_tok[:, None] * out_grad.astype(jnp.float32)).astype(jnp.bfloat16)
    chosen = expert_ids.reshape(-1)
    pairs = chosen.shape[0]
    onehot = chosen[:, None] == jnp.arange(experts, dtype=jnp.int32)[None, :]
    rank = jnp.arange(pairs, dtype=jnp.int32)
    lower = (rank[None, :] < rank[:, None]).astype(jnp.bfloat16)
    earlier = jnp.dot(lower, onehot.astype(jnp.bfloat16), preferred_element_type=jnp.float32)
    position = jnp.sum(jnp.where(onehot, earlier, 0.0), axis=1).astype(jnp.int32)
    slot_index = chosen * capacity + position
    filled = slot_index[None, :] == jnp.arange(block_size, dtype=jnp.int32)[:, None]
    send_probs = jnp.sum(
        jnp.where(filled, route_probs.reshape(-1).astype(jnp.float32)[None, :], 0.0), axis=1
    )
    by_token = slot_index.reshape(token_count, 2)
    every = jnp.arange(block_size, dtype=jnp.int32)[:, None]
    picks = ((by_token[:, 0][None, :] == every) | (by_token[:, 1][None, :] == every)).astype(
        jnp.bfloat16
    )
    send_rows = jnp.dot(picks, scaled, preferred_element_type=jnp.float32).astype(jnp.bfloat16)
    prob_tile = jnp.zeros((experts, SUBLANES, padded), jnp.float32)
    prob_tile = prob_tile + jnp.pad(
        send_probs.reshape(experts, 1, capacity), ((0, 0), (0, 0), (0, padded - capacity))
    )
    amount = copy_count(columns, experts, cores)
    gathered, probs_all = pl.pallas_call(
        functools.partial(gather_kernel, columns, experts, cores),
        out_shape=(
            jax.ShapeDtypeStruct((columns, experts, capacity, width), jnp.bfloat16),
            jax.ShapeDtypeStruct((columns, experts, SUBLANES, padded), jnp.float32),
        ),
        in_specs=[pl.BlockSpec(memory_space=pltpu.VMEM)] * 2,
        out_specs=[pl.BlockSpec(memory_space=pltpu.VMEM)] * 2,
        scratch_shapes=[pltpu.SemaphoreType.DMA((amount,)), pltpu.SemaphoreType.DMA((amount,))],
        compiler_params=pltpu.CompilerParams(
            collective_id=0, has_side_effects=True, vmem_limit_bytes=40 * 1024 * 1024
        ),
        name="gather",
    )(send_rows.reshape(experts, capacity, half_width), prob_tile)
    gathered = gathered.reshape(slots, width)
    arrived_probs = probs_all[:, :, 0, :capacity].reshape(slots)

    gate_piece = gate_local.astype(jnp.float32)
    up_piece = up_local.astype(jnp.float32)
    activated, derivative = silu_parts(gate_piece)
    hidden = (activated * up_piece).astype(jnp.bfloat16)
    upstream = lax.dot_general(
        weight_local, gathered, (((1,), (1,)), ((), ())), preferred_element_type=jnp.float32
    )
    partial_value = jnp.sum(upstream * hidden.astype(jnp.float32), axis=0)
    grad_hidden = arrived_probs[None, :] * upstream
    gate_out = (grad_hidden * up_piece * derivative).astype(jnp.bfloat16)
    up_out = (grad_hidden * activated).astype(jnp.bfloat16)
    weighted = (arrived_probs[:, None] * gathered.astype(jnp.float32)).astype(jnp.bfloat16)
    grad_w = jnp.dot(hidden, weighted, preferred_element_type=jnp.float32).astype(jnp.bfloat16)

    parts = jnp.pad(
        partial_value.reshape(columns, experts, capacity),
        ((0, 0), (0, depth - experts), (0, padded - capacity)),
    )
    firsts = columns * cores - 1
    number = firsts + experts - 1
    totals = pl.pallas_call(
        functools.partial(probe_kernel, columns, experts, cores),
        out_shape=jax.ShapeDtypeStruct((depth, padded), jnp.float32),
        in_specs=[pl.BlockSpec(memory_space=pltpu.VMEM)],
        out_specs=pl.BlockSpec(memory_space=pltpu.VMEM),
        scratch_shapes=[
            pltpu.VMEM((firsts, depth, padded), jnp.float32),
            pltpu.VMEM((depth, padded), jnp.float32),
            pltpu.VMEM((experts - 1, depth, padded), jnp.float32),
            pltpu.SemaphoreType.DMA((number,)),
            pltpu.SemaphoreType.DMA((number,)),
        ],
        compiler_params=pltpu.CompilerParams(collective_id=1, has_side_effects=True),
        name="probe",
    )(parts)
    returned = totals[:experts, :capacity].reshape(-1)
    grad_probs = jnp.sum(jnp.where(filled, returned[:, None], 0.0), axis=0).reshape(token_count, 2)
    return (gate_out[None], up_out[None], grad_w[None], grad_probs)


def solution(mesh):
    return jax.shard_map(
        local,
        mesh=mesh,
        in_specs=(
            P(("dp", "expert"), "tensor"),
            P(("dp", "expert"), None),
            P(("dp", "expert"), None),
            P(("dp", "expert"), None),
            P(("dp", "expert"), None),
            P("expert", ("dp", "tensor"), None),
            P("expert", ("dp", "tensor"), None),
            P("expert", ("dp", "tensor"), None),
        ),
        out_specs=(
            P("expert", ("dp", "tensor"), None),
            P("expert", ("dp", "tensor"), None),
            P("expert", ("dp", "tensor"), None),
            P(("dp", "expert"), None),
        ),
        check_vma=False,
    )
```

```python
import functools

import jax
import jax.numpy as jnp
from jax import lax
from jax.experimental import pallas as pl
from jax.experimental.pallas import tpu as pltpu
from jax.sharding import PartitionSpec as P

MESH = pl.DeviceIdType.MESH
LANES = 128
SUBLANES = 8


def silu_parts(pre_act):
    logistic = jax.nn.sigmoid(pre_act)
    return (pre_act * logistic, logistic * (1.0 + pre_act * (1.0 - logistic)))


def flip(index, mask):
    bit = 1
    while bit <= mask:
        if mask & bit:
            index = index + bit * (1 - 2 * lax.rem(lax.div(index, bit), 2))
        bit *= 2
    return index


class Copies:
    def __init__(self, send_sem, recv_sem):
        self.send_sem, self.recv_sem, self.made = send_sem, recv_sem, []

    def start(self, src, dst, device):
        at = len(self.made)
        copy = pltpu.make_async_remote_copy(
            src_ref=src,
            dst_ref=dst,
            send_sem=self.send_sem.at[at],
            recv_sem=self.recv_sem.at[at],
            device_id=device,
            device_id_type=MESH,
        )
        copy.start()
        self.made.append(copy)
        return copy


def greet(peers):
    barrier = pltpu.get_barrier_semaphore()
    for peer in peers:
        pl.semaphore_signal(barrier, inc=1, device_id=peer, device_id_type=MESH)
    pl.semaphore_wait(barrier, len(peers))


def copy_count(columns, experts, cores):
    probe = columns * cores + experts
    if columns == 4:
        per_block = 6 + 7 * (cores - 1)
        return (experts - 1) * 2 + (columns - 1) + experts * per_block + probe
    return (experts - 1) * 2 + (columns - 1) * 2 + columns * (cores - 1) + probe


def row_tile(rows):
    return max(tile for tile in range(16, 257, 16) if rows % tile == 0)


def moe_kernel(
    columns,
    experts,
    cores,
    rows_ref,
    probs_ref,
    weight_hbm,
    gate_hbm,
    up_hbm,
    ups_ref,
    acc_ref,
    probs_out,
    probe_out,
    gathered,
    weight_ref,
    gate_ref,
    up_ref,
    hidden_ref,
    weighted_ref,
    part_ref,
    first,
    total,
    second,
    load_sem,
    send_sem,
    recv_sem,
):
    d, e, t = lax.axis_index("dp"), lax.axis_index("expert"), lax.axis_index("tensor")
    capacity, half = rows_ref.shape[1], rows_ref.shape[2]
    group_size = experts * capacity
    units = weight_ref.shape[0]
    tile = row_tile(units)
    tiles = units // tile
    loads = [
        pltpu.make_async_copy(src, dst, load_sem.at[at])
        for at, (src, dst) in enumerate(
            ((gate_hbm, gate_ref), (up_hbm, up_ref), (weight_hbm, weight_ref))
        )
    ]
    for load in loads:
        load.start()
    greet(
        [(d, flip(e, k), t) for k in range(1, experts)]
        + [
            (flip(d, m), e, flip(t, f))
            for m in range(columns)
            for f in range(cores)
            if m or f
        ]
    )
    copies = Copies(send_sem, recv_sem)
    base = pl.multiple_of(t * half, half)
    mine = pl.ds(base, half)
    along, small = [None], [None]
    for k in range(1, experts):
        to = (d, flip(e, k), t)
        along.append(copies.start(rows_ref.at[flip(e, k)], gathered.at[d, e, :, mine], to))
        small.append(copies.start(probs_ref.at[flip(e, k)], probs_out.at[d, e], to))
    last = [[] for _ in range(columns)]

    def to_cores(m, src, dst):
        for f in range(1, cores):
            last[m].append(copies.start(src, dst, (d, e, flip(t, f))))

    def make_hidden(at):
        if at == 0:
            loads[0].wait()
            loads[1].wait()
        span = pl.ds(at * tile, tile)
        gate = gate_ref[span, :].astype(jnp.float32)
        hidden_ref[span, :] = (gate * jax.nn.sigmoid(gate) * up_ref[span, :].astype(jnp.float32)).astype(
            jnp.bfloat16
        )

    def some_hidden(k):
        for at in range(k * tiles // experts, (k + 1) * tiles // experts):
            make_hidden(at)

    def spread_probs():
        for k in range(1, experts):
            small[k].wait_recv()
        group = probs_out.at[d]
        for m in range(1, columns):
            last[m].append(copies.start(group, group, (flip(d, m), e, t)))

    firsts = {}

    def compute(m):
        for copy in last[m]:
            copy.wait_recv()
        where = flip(d, m)
        cols = pl.ds(pl.multiple_of(where * group_size, 128), group_size)
        eye = lax.broadcasted_iota(jnp.int32, (capacity, capacity), 0) == lax.broadcasted_iota(
            jnp.int32, (capacity, capacity), 1
        )
        for j in range(experts):
            prob = probs_out[where, j][0:1, 0:capacity]
            diag = jnp.where(eye, prob, 0.0).astype(jnp.bfloat16)
            weighted_ref[pl.ds(j * capacity, capacity), :] = jnp.dot(
                diag, gathered[where, j], preferred_element_type=jnp.float32
            ).astype(jnp.bfloat16)

        def up_step(i, part):
            span = pl.ds(pl.multiple_of(i * tile, tile), tile)
            block = gathered[where].reshape(group_size, half * cores)
            ups = lax.dot_general(
                weight_ref[span, :], block, (((1,), (1,)), ((), ())),
                preferred_element_type=jnp.float32,
            )
            ups_ref[span, cols] = ups
            value = ups * hidden_ref[span, cols].astype(jnp.float32)
            return part + jnp.sum(value, axis=0, keepdims=True)

        part = lax.fori_loop(0, tiles, up_step, jnp.zeros((1, group_size), jnp.float32))
        part_ref[where] = jnp.broadcast_to(part, (8, group_size))
        for f in range(cores):
            if m or f:
                at = m * cores + f - 1
                firsts[at] = copies.start(
                    part_ref.at[where], first.at[at], (where, e, flip(t, f))
                )

        def down_step(i, carry):
            span = pl.ds(pl.multiple_of(i * tile, tile), tile)
            out = jnp.dot(
                hidden_ref[span, cols], weighted_ref[...], preferred_element_type=jnp.float32
            )
            acc_ref[span, :] = out if m == 0 else acc_ref[span, :] + out
            return carry

        lax.fori_loop(0, tiles, down_step, 0)

    if columns == 4:
        piece = half // 2
        cuts = [pl.ds(pl.multiple_of(base + p * piece, piece), piece) for p in range(2)]
        sent = {}

        def spread(k):
            origin = flip(e, k)
            if k > 0:
                along[k].wait_recv()
            for m, order in ((1, (0, 1)), (2, (1, 0))):
                for p in order:
                    here = gathered.at[d, origin, :, cuts[p]]
                    src = rows_ref.at[e, :, pl.ds(p * piece, piece)] if k == 0 else here
                    sent[k, m, p] = copies.start(src, here, (flip(d, m), e, t))
            whole = gathered.at[d, origin, :, mine]
            to_cores(0, rows_ref.at[e] if k == 0 else whole, whole)

        def forward(k):
            origin = flip(e, k)
            for m, p in ((1, 0), (2, 1)):
                sent[k, m, p].wait_recv()
                block = gathered.at[flip(d, m), origin, :, cuts[p]]
                sent[k, 3, p] = copies.start(block, block, (flip(d, 3 - m), e, t))
                to_cores(m, block, block)
            for m, p in ((1, 1), (2, 0)):
                sent[k, m, p].wait_recv()
                block = gathered.at[flip(d, m), origin, :, cuts[p]]
                to_cores(m, block, block)

        def finish(k):
            for p in range(2):
                sent[k, 3, p].wait_recv()
                block = gathered.at[flip(d, 3), flip(e, k), :, cuts[p]]
                to_cores(3, block, block)

        spread(0)
        gathered[d, e, :, mine] = rows_ref[e]
        probs_out[d, e] = probs_ref[e]
        some_hidden(0)
        for k in range(1, experts):
            spread(k)
            some_hidden(k)
            if k == 1:
                forward(0)
        spread_probs()
        for k in range(1, experts - 1):
            forward(k)
        loads[2].wait()
        compute(0)
        forward(experts - 1)
        compute(1)
        for k in range(experts - 1):
            finish(k)
        compute(2)
        finish(experts - 1)
        compute(3)
    else:
        gathered[d, e, :, mine] = rows_ref[e]
        probs_out[d, e] = probs_ref[e]
        for k in range(1, experts):
            along[k].wait_recv()
        group = gathered.at[d, :, :, mine]
        spreads = [copies.start(group, group, (flip(d, m), e, t)) for m in range(1, columns)]
        to_cores(0, group, group)
        spread_probs()
        for at in range(tiles):
            make_hidden(at)
        loads[2].wait()
        compute(0)
        for m in range(1, columns):
            spreads[m - 1].wait_recv()
            block = gathered.at[flip(d, m), :, :, mine]
            to_cores(m, block, block)
            compute(m)
    acc = part_ref[d]
    for at in range(columns * cores - 1):
        firsts[at].wait_recv()
        acc = acc + first[at]
    total[...] = acc
    backs = [copies.start(total, second.at[k - 1], (d, flip(e, k), t)) for k in range(1, experts)]
    probe_out[e] = acc
    for k in range(1, experts):
        backs[k - 1].wait_recv()
        probe_out[flip(e, k)] = second[k - 1]
    for copy in copies.made:
        copy.wait_send()


def local(out_grad, seq_ids, seq_weights, expert_ids, route_probs, down_weight, gate_pre, up_pre):
    experts = lax.axis_size("expert")
    columns = lax.axis_size("dp")
    cores = lax.axis_size("tensor")
    token_count = seq_ids.shape[1]
    slots = gate_pre.shape[2]
    capacity = slots // (columns * experts)
    half_width = out_grad.shape[1]
    width = half_width * cores
    seq_count = seq_weights.shape[1]
    block_size = experts * capacity
    padded = -(-capacity // LANES) * LANES
    gate_local = gate_pre[0]
    up_local = up_pre[0]
    weight_local = down_weight[0]
    member = (seq_ids[0][:, None] == jnp.arange(seq_count, dtype=jnp.int32)[None, :]).astype(
        jnp.float32
    )
    weight_tok = jnp.sum(member * seq_weights[0][None, :], axis=1)
    scaled = (weight_tok[:, None] * out_grad.astype(jnp.float32)).astype(jnp.bfloat16)
    chosen = expert_ids.reshape(-1)
    pairs = chosen.shape[0]
    onehot = chosen[:, None] == jnp.arange(experts, dtype=jnp.int32)[None, :]
    rank = jnp.arange(pairs, dtype=jnp.int32)
    lower = (rank[None, :] < rank[:, None]).astype(jnp.bfloat16)
    earlier = jnp.dot(lower, onehot.astype(jnp.bfloat16), preferred_element_type=jnp.float32)
    position = jnp.sum(jnp.where(onehot, earlier, 0.0), axis=1).astype(jnp.int32)
    slot_index = chosen * capacity + position
    filled = slot_index[None, :] == jnp.arange(block_size, dtype=jnp.int32)[:, None]
    send_probs = jnp.sum(
        jnp.where(filled, route_probs.reshape(-1).astype(jnp.float32)[None, :], 0.0), axis=1
    )
    by_token = slot_index.reshape(token_count, 2)
    every = jnp.arange(block_size, dtype=jnp.int32)[:, None]
    picks = ((by_token[:, 0][None, :] == every) | (by_token[:, 1][None, :] == every)).astype(
        jnp.bfloat16
    )
    send_rows = jnp.dot(picks, scaled, preferred_element_type=jnp.float32).astype(jnp.bfloat16)
    prob_tile = jnp.zeros((experts, SUBLANES, padded), jnp.float32)
    prob_tile = prob_tile + jnp.pad(
        send_probs.reshape(experts, 1, capacity), ((0, 0), (0, 0), (0, padded - capacity))
    )
    amount = copy_count(columns, experts, cores)
    units = weight_local.shape[0]
    anywhere = pl.BlockSpec(memory_space=pl.ANY)
    inside = pl.BlockSpec(memory_space=pltpu.VMEM)
    upstream, grad_w, probs_all, probes = pl.pallas_call(
        functools.partial(moe_kernel, columns, experts, cores),
        out_shape=(
            jax.ShapeDtypeStruct((units, slots), jnp.float32),
            jax.ShapeDtypeStruct((units, width), jnp.float32),
            jax.ShapeDtypeStruct((columns, experts, SUBLANES, padded), jnp.float32),
            jax.ShapeDtypeStruct((experts, SUBLANES, block_size), jnp.float32),
        ),
        in_specs=[inside, inside, anywhere, anywhere, anywhere],
        out_specs=[inside] * 4,
        scratch_shapes=[
            pltpu.VMEM((columns, experts, capacity, width), jnp.bfloat16),
            pltpu.VMEM((units, width), jnp.bfloat16),
            pltpu.VMEM((units, slots), jnp.bfloat16),
            pltpu.VMEM((units, slots), jnp.bfloat16),
            pltpu.VMEM((units, slots), jnp.bfloat16),
            pltpu.VMEM((block_size, width), jnp.bfloat16),
            pltpu.VMEM((columns, SUBLANES, block_size), jnp.float32),
            pltpu.VMEM((columns * cores - 1, SUBLANES, block_size), jnp.float32),
            pltpu.VMEM((SUBLANES, block_size), jnp.float32),
            pltpu.VMEM((experts - 1, SUBLANES, block_size), jnp.float32),
            pltpu.SemaphoreType.DMA((3,)),
            pltpu.SemaphoreType.DMA((amount,)),
            pltpu.SemaphoreType.DMA((amount,)),
        ],
        compiler_params=pltpu.CompilerParams(
            collective_id=0, has_side_effects=True, vmem_limit_bytes=50 * 1024 * 1024
        ),
        name="moe",
    )(send_rows.reshape(experts, capacity, half_width), prob_tile, weight_local, gate_local, up_local)
    arrived_probs = probs_all[:, :, 0, :capacity].reshape(slots)
    gate_piece = gate_local.astype(jnp.float32)
    up_piece = up_local.astype(jnp.float32)
    activated, derivative = silu_parts(gate_piece)
    grad_hidden = arrived_probs[None, :] * upstream
    gate_out = (grad_hidden * up_piece * derivative).astype(jnp.bfloat16)
    up_out = (grad_hidden * activated).astype(jnp.bfloat16)
    grad_w = grad_w.astype(jnp.bfloat16)
    own = lax.dynamic_slice_in_dim(
        probes[:, 0, :], lax.axis_index("expert") * capacity, capacity, 1
    )
    returned = own.reshape(-1)
    grad_probs = jnp.sum(jnp.where(filled, returned[:, None], 0.0), axis=0).reshape(token_count, 2)
    return (gate_out[None], up_out[None], grad_w[None], grad_probs)


def solution(mesh):
    return jax.shard_map(
        local,
        mesh=mesh,
        in_specs=(
            P(("dp", "expert"), "tensor"),
            P(("dp", "expert"), None),
            P(("dp", "expert"), None),
            P(("dp", "expert"), None),
            P(("dp", "expert"), None),
            P("expert", ("dp", "tensor"), None),
            P("expert", ("dp", "tensor"), None),
            P("expert", ("dp", "tensor"), None),
        ),
        out_specs=(
            P("expert", ("dp", "tensor"), None),
            P("expert", ("dp", "tensor"), None),
            P("expert", ("dp", "tensor"), None),
            P(("dp", "expert"), None),
        ),
        check_vma=False,
    )
```
